32 devices in a mesh: row: 8 (over y, x, core), col: 4 (over z).
Axes of the slice: x: 2, y: 2, z: 4, core: 2. Of those that a mesh axis runs over, the one named last changes fastest.
Arguments:
- ctrl_start: float32 [16384, 512], P(('row', 'col')), may hold values from -6 to 6
- obsv_start: float32 [16384, 512], P(('row', 'col')), may hold values from -6 to 6
- band_tiles: float32 [16384, 384], P(('row', 'col')), may hold values from -0.15625 to 0.15625
- band_offsets: int32 [128, 3], P(('row', 'col')), may hold values from -2 to 2, as said below
Outputs:
- cross_product: float32 [2048, 2048], P('row', 'col')
The draws below stay inside these ranges and needn't reach their ends.
Inputs may be any that keep to these rules, and one draw needn't show every extreme that they name: `band_offsets`: the 3 offsets of a tile row are distinct.
All inputs are finite; a program needn't handle non-finite values.
Results may differ from the reference program's by a relative error of at most 0.0003.
Values sent between devices are 32-bit elements; how exact they have to be, the bound alone decides.
No kernel may reach another device: no remote copies, remote signals or barrier semaphores. Data moves between devices by JAX's collectives and lax.ppermute only.
A program may use at most 128 MiB of HBM per device.

```python
import math
import jax
import jax.numpy as jnp
from jax import lax

TILE = 128
HALO = 2
BAND = 3
INIT_COLS = 512
ORDER = 16384
NTILES = 128


def draw_band_offsets(key, part):
    width = 2 * HALO + 1
    scores = jax.random.randint(jax.random.fold_in(key, 17), (NTILES, width), 0, 1 << 20) * 8 + jnp.arange(width, dtype=jnp.int32)
    picked = jnp.argsort(scores, axis=1)[:, :BAND]
    return (picked - HALO).astype(jnp.int32)


def level_of(key, shape, split, smallest, largest):
    loudness, own = 1.0, jax.random.fold_in(key, 6)
    for position, blocks in split:
        heights = jnp.exp(jax.random.uniform(jax.random.fold_in(own, position), (blocks,), jnp.float32, smallest / len(split), largest / len(split)))
        loudness = loudness * jnp.repeat(heights, shape[position] // blocks).reshape([-1 if axis == position else 1 for axis in range(len(shape))])
    return loudness


def gaussian(key, dims, spread, limit, cuts=(), kind=jnp.bfloat16):
    gain = level_of(key, dims, cuts, -0.22, 0.18) if cuts else 1.0
    entries = jax.random.normal(key, dims, jnp.float32) * spread * gain
    return jnp.minimum(jnp.maximum(entries, -limit), limit).astype(kind)


def setup_inputs(seed: int = 0) -> dict:
    key_of = jax.random.split(jax.random.key(seed), 5)
    return {
        "ctrl_start": gaussian(key_of[0], (ORDER, INIT_COLS), 1.0, 6.0, ((0, 32),), jnp.float32),
        "obsv_start": gaussian(key_of[1], (ORDER, INIT_COLS), 1.0, 6.0, ((0, 32),), jnp.float32),
        "band_tiles": gaussian(key_of[2], (ORDER, BAND * TILE), (4 * BAND * TILE) ** -0.5, 0.15625, ((0, 32),), jnp.float32),
        "band_offsets": draw_band_offsets(jax.random.fold_in(key_of[4], 71), 0),
    }


def forward(field, tiles, offsets):
    count = field.shape[0] // TILE
    margin = HALO * TILE
    padded = jnp.pad(field, ((margin, margin), (0, 0)))

    def one_row(index):
        parts = []
        for slot in range(BAND):
            start = ((index + offsets[index, slot]) * TILE + margin).astype(jnp.int32)
            parts.append(lax.dynamic_slice_in_dim(padded, start, TILE, 0))
        stacked = jnp.concatenate(parts, 0)
        tile_row = lax.dynamic_slice_in_dim(tiles, (index * TILE).astype(jnp.int32), TILE, 0)
        return jnp.dot(tile_row, stacked, precision=lax.Precision.HIGHEST, preferred_element_type=jnp.float32)
    result = lax.map(one_row, jnp.arange(count, dtype=jnp.int32))
    return result.reshape(field.shape[0], field.shape[1])

def transpose(field, tiles, offsets):
    total = field.shape[0]
    count = total // TILE
    margin = HALO * TILE
    padded = jnp.zeros((total + 2 * margin, field.shape[1]), jnp.float32)

    def step(index, acc):
        index = jnp.asarray(index).astype(jnp.int32)
        piece = lax.dynamic_slice_in_dim(field, index * TILE, TILE, 0)
        tile_row = lax.dynamic_slice_in_dim(tiles, index * TILE, TILE, 0)
        terms = jnp.dot(tile_row.T, piece, precision=lax.Precision.HIGHEST, preferred_element_type=jnp.float32)
        for slot in range(BAND):
            start = ((index + offsets[index, slot]) * TILE + margin).astype(jnp.int32)
            current = lax.dynamic_slice_in_dim(acc, start, TILE, 0)
            acc = lax.dynamic_update_slice_in_dim(acc, current + terms[slot * TILE:(slot + 1) * TILE], start, 0)
        return acc
    padded = lax.fori_loop(0, count, step, padded)
    return padded[margin:margin + total]

def reference(ctrl_start, obsv_start, band_tiles, band_offsets):
    ctrl_one = jnp.concatenate([ctrl_start, forward(ctrl_start, band_tiles, band_offsets)], 1)
    ctrl_two = jnp.concatenate([ctrl_one, forward(forward(ctrl_one, band_tiles, band_offsets), band_tiles, band_offsets)], 1)
    obsv_one = jnp.concatenate([obsv_start, transpose(obsv_start, band_tiles, band_offsets)], 1)
    obsv_two = jnp.concatenate([obsv_one, transpose(transpose(obsv_one, band_tiles, band_offsets), band_tiles, band_offsets)], 1)
    product = jnp.dot(obsv_two.T, ctrl_two, precision=lax.Precision.HIGHEST, preferred_element_type=jnp.float32)
    return product * (1.0 / math.sqrt(ORDER))
```

```python
import functools
import math

import jax
import jax.numpy as jnp
from jax import lax
from jax.experimental import pallas as pl
from jax.experimental.pallas import tpu as pltpu
from jax.sharding import PartitionSpec as P

TILE = 128
HALO = 2
BAND = 3
ORDERS = 4
AXES = ("row", "col")
VMEM = pltpu.VMEM
GROUPS = ((0, 1, 2), (3, 4, 5), (6,))


def call(kernel, outs, ins, scratch=(), flops=0, bytes_=0, scalars=0):
    specs = [pl.BlockSpec(memory_space=pltpu.SMEM)] * scalars
    specs += [pl.BlockSpec(memory_space=VMEM)] * (len(ins) - scalars)
    return pl.pallas_call(
        kernel,
        out_shape=outs,
        in_specs=specs,
        out_specs=jax.tree.map(lambda _: pl.BlockSpec(memory_space=VMEM), outs),
        scratch_shapes=list(scratch),
        cost_estimate=pl.CostEstimate(flops=flops, bytes_accessed=bytes_, transcendentals=0),
    )(*ins)


def split(value):
    high = value.astype(jnp.bfloat16)
    return high, (value - high.astype(jnp.float32)).astype(jnp.bfloat16)


def dot(a, b):
    return jnp.dot(a, b, preferred_element_type=jnp.float32)


def forward_kernel(offs, before, top, bottom, after, tiles, top_out, bottom_out, high, low):
    margin = HALO * TILE
    for place, ref in enumerate((before, top, bottom, after)):
        here = pl.ds(place * margin, margin)
        high[here, :], low[here, :] = split(ref[...])
    for index in range(2 * HALO):
        starts = [pl.multiple_of((index + HALO + offs[index, b]) * TILE, TILE) for b in range(BAND)]
        stack_high = jnp.concatenate([high[pl.ds(s, TILE), :] for s in starts], 0)
        stack_low = jnp.concatenate([low[pl.ds(s, TILE), :] for s in starts], 0)
        tile_high, tile_low = split(tiles[index * TILE : (index + 1) * TILE, :])
        result = dot(tile_high, stack_high) + (dot(tile_high, stack_low) + dot(tile_low, stack_high))
        out, at = (top_out, index) if index < HALO else (bottom_out, index - HALO)
        out[at * TILE : (at + 1) * TILE, :] = result


def forward(offs, before, top, bottom, after, tiles):
    shape = jax.ShapeDtypeStruct(top.shape, jnp.float32)
    rows, width = 2 * top.shape[0], top.shape[1]
    scratch = [VMEM((2 * rows, width), jnp.bfloat16)] * 2
    return call(
        forward_kernel, (shape, shape), (offs, before, top, bottom, after, tiles), scratch,
        6 * rows * BAND * TILE * width, 4 * (4 * rows * width), 1,
    )


def turn_kernel(parts, quarters, pos, obsv, high_out, low_out):
    high, low = split(obsv[...].T)
    width = high.shape[0] // (parts * quarters)
    for d in range(parts):
        for e in range(quarters):
            for p in range(parts):
                for q in range(quarters):
                    @pl.when(jnp.logical_and((pos[0] + d) % parts == p, (pos[1] + e) % quarters == q))
                    def _(d=d, e=e, p=p, q=q):
                        here = (d * quarters + e) * width
                        there = (p * quarters + q) * width
                        high_out[here : here + width, :] = high[there : there + width]
                        low_out[here : here + width, :] = low[there : there + width]


def product_kernel(high, low, top, bottom, *outs):
    half = top.shape[0]
    right_high, right_low = split(jnp.concatenate([top[...], bottom[...]], 0))
    rows = high.shape[0] // len(outs)
    for d, out in enumerate(outs):
        here = pl.ds(d * rows, rows)
        a = high[here, :]
        out[...] = dot(a, right_high) + (dot(a, right_low) + dot(low[here, :], right_high))


def product(high, low, top, bottom, parts):
    rows, width = high.shape[0], top.shape[1]
    shapes = tuple(jax.ShapeDtypeStruct((rows // parts, width), jnp.float32) for _ in range(parts))
    return call(
        product_kernel, shapes, (high, low, top, bottom), (),
        6 * rows * width * high.shape[1], 4 * 4 * rows * width,
    )


def pick_kernel(count, pos, *refs):
    sources, outs = refs[: -count], refs[-count:]
    for d, out in enumerate(outs):
        power = (pos[1] + d) % count + pos[2]
        for k, ref in enumerate(sources):
            @pl.when(power == k)
            def _(out=out, ref=ref):
                out[...] = ref[...]


def place_kernel(scale, pos, *refs):
    *parts, out = refs
    count = len(parts)
    rows = parts[0].shape[0]
    for d, ref in enumerate(parts):
        at = (pos[1] + count - d) % count
        out[pl.ds(pl.multiple_of(at * rows, rows), rows), :] = ref[...] * scale


def local(rows_all, cols_all, ctrl, obsv, tiles, offs):
    total = rows_all * cols_all
    parts, splits = rows_all // ORDERS, cols_all // ORDERS
    r, c = lax.axis_index("row"), lax.axis_index("col")
    big_row, part, big_col, piece = r // parts, r % parts, c // splits, c % splits
    pos = jnp.stack([part, big_row, big_col, piece]).astype(jnp.int32)
    devices = [(i, j) for i in range(rows_all) for j in range(cols_all)]

    def flat(i, j):
        return i * cols_all + j

    def permute(x, pairs):
        return lax.ppermute(x, AXES, pairs)

    def peers(move):
        return [(flat(i, j), flat(*move(i, j))) for i, j in devices]

    def seat(s):
        lane, q = divmod(s, 2 * cols_all)
        j = q // 2 if lane % 2 == 0 else cols_all - 1 - q // 2
        return flat(2 * lane + q % 2, j)

    seats = [seat(s) for s in range(total)]
    relay = [(s, seats[s]) for s in range(total)]
    up = [(seats[s], seats[s + 1]) for s in range(total - 1)]
    down = [(b, a) for a, b in up]

    margin = HALO * TILE
    width = ctrl.shape[1]
    offs = permute(offs, relay)
    top, bottom = permute(ctrl[:margin], relay), permute(ctrl[margin:], relay)
    tiles = permute(tiles, relay)
    obsv = permute(obsv, relay)
    quarter = width // (parts * ORDERS)
    half = jax.ShapeDtypeStruct((width, obsv.shape[0]), jnp.bfloat16)
    high, low = call(
        functools.partial(turn_kernel, parts, ORDERS), (half, half), (pos, obsv), (),
        width * width, 8 * width * width, 1,
    )

    def over_parts(blocks):
        kept = blocks[0]
        for d in range(1, parts):
            kept = kept + permute(
                blocks[d], peers(lambda i, j: ((i // parts) * parts + (i + d) % parts, j))
            )
        if splits == 1:
            return kept
        wide = kept.shape[1] // splits
        cut = [
            lax.dynamic_slice_in_dim(kept, ((piece + d) % splits) * wide, wide, 1)
            for d in range(splits)
        ]
        kept = cut[0]
        for d in range(1, splits):
            kept = kept + permute(
                cut[d], peers(lambda i, j: (i, (j // splits) * splits + (j + d) % splits))
            )
        return kept

    def turned(i, e):
        return ((i // parts + e) % ORDERS) * parts + i % parts

    def over_rows(block):
        kept = block[:, :quarter]
        for e in range(1, ORDERS):
            sent = block[:, e * quarter : (e + 1) * quarter]
            kept = kept + permute(sent, peers(lambda i, j: (turned(i, e), j)))
        return kept

    def line(moves):
        return [
            (flat(i, a * splits + s), flat(i, b * splits + s))
            for a, b in moves for i in range(rows_all) for s in range(splits)
        ]

    def over_cols(own, powers):
        low_k, high_k = min(powers), max(powers)
        last = 2 * ORDERS - 2
        first = []
        if high_k >= 1:
            first.append((0, 1))
        if low_k < last:
            first.append((3, 2))
        second = []
        if high_k >= 2:
            second.append((1, 2))
        if low_k <= last - 2:
            second.append((2, 1))
        third = []
        if low_k <= ORDERS - 1:
            third.append((1, 0))
        if high_k >= ORDERS - 1:
            third.append((2, 3))
        both = own + permute(own, line(first))
        both = both + permute(both, line(second))
        ends = permute(both, line(third))
        if (3, 2) not in first:
            ends = ends + jnp.where(big_col == 3, own, 0.0)
        outer = jnp.logical_or(big_col == 0, big_col == 3)
        return jnp.where(outer, ends, both)

    powers = {}
    kept = {}
    for group in GROUPS:
        sums = []
        for k in group:
            if k > 0:
                before, after = permute(bottom, up), permute(top, down)
                top, bottom = forward(offs, before, top, bottom, after, tiles)
            sums.append(over_parts(product(high, low, top, bottom, parts)))
        own = over_rows(jnp.stack(sums))
        done = over_cols(own, group)
        for at, k in enumerate(group):
            kept[k] = done[at]

    shape = kept[0].shape
    block = jax.ShapeDtypeStruct(shape, jnp.float32)
    sent = call(
        functools.partial(pick_kernel, ORDERS), (block,) * ORDERS,
        (pos, *[kept[k] for k in range(2 * ORDERS - 1)]), (), shape[0] * shape[1], 44 * shape[0] * shape[1], 1,
    )
    got = [sent[0]] + [permute(sent[d], peers(lambda i, j: (turned(i, d), j))) for d in range(1, ORDERS)]
    out = jax.ShapeDtypeStruct((ORDERS * shape[0], shape[1]), jnp.float32)
    scale = 1.0 / math.sqrt(ctrl.shape[0] * total)
    return call(
        functools.partial(place_kernel, scale), out, (pos, *got), (),
        shape[0] * shape[1], 32 * shape[0] * shape[1], 1,
    )


def solution(mesh):
    return jax.shard_map(
        functools.partial(local, mesh.shape["row"], mesh.shape["col"]),
        mesh=mesh,
        in_specs=(P(AXES, None),) * 4,
        out_specs=P("row", "col"),
        check_vma=False,
    )
```

```python
import functools
import math

import jax
import jax.numpy as jnp
from jax import lax
from jax.experimental import pallas as pl
from jax.experimental.pallas import tpu as pltpu
from jax.sharding import PartitionSpec as P

TILE = 128
HALO = 2
BAND = 3
ORDERS = 4
AXES = ("row", "col")
VMEM = pltpu.VMEM
GRANT = 16 * 2**20
ROW_GROUPS = ((0,), (1, 2), (3, 4), (5,), (6,))
COL_GROUPS = ((0, 1, 2), (3, 4, 5), (6,))


def call(kernel, outs, ins, scratch=(), flops=0, bytes_=0, scalars=0):
    specs = [pl.BlockSpec(memory_space=pltpu.SMEM)] * scalars
    specs += [pl.BlockSpec(memory_space=VMEM)] * (len(ins) - scalars)
    return pl.pallas_call(
        kernel,
        out_shape=outs,
        in_specs=specs,
        out_specs=jax.tree.map(lambda _: pl.BlockSpec(memory_space=VMEM), outs),
        scratch_shapes=list(scratch),
        cost_estimate=pl.CostEstimate(flops=flops, bytes_accessed=bytes_, transcendentals=0),
        compiler_params=pltpu.CompilerParams(vmem_limit_bytes=GRANT),
    )(*ins)


def split(value):
    high = value.astype(jnp.bfloat16)
    return high, (value - high.astype(jnp.float32)).astype(jnp.bfloat16)


def dot(a, b):
    return jnp.dot(a, b, preferred_element_type=jnp.float32)


def forward_kernel(offs, pos, outer, inner, from_outer, from_inner, tiles, outer_out, inner_out, high, low):
    margin = HALO * TILE
    odd = pos[4]
    placed = ((from_outer, 3 * odd), (outer, 1 + odd), (inner, 2 - odd), (from_inner, 3 - 3 * odd))
    for ref, place in placed:
        here = pl.ds(pl.multiple_of(place * margin, margin), margin)
        high[here, :], low[here, :] = split(ref[...])
    for out, base in ((outer_out, HALO * odd), (inner_out, HALO * (1 - odd))):
        for i in range(HALO):
            index = base + i
            starts = [
                pl.multiple_of((index + HALO + offs[index, b]) * TILE, TILE) for b in range(BAND)
            ]
            stack_high = jnp.concatenate([high[pl.ds(s, TILE), :] for s in starts], 0)
            stack_low = jnp.concatenate([low[pl.ds(s, TILE), :] for s in starts], 0)
            tile_high, tile_low = split(tiles[pl.ds(pl.multiple_of(index * TILE, TILE), TILE), :])
            out[i * TILE : (i + 1) * TILE, :] = dot(tile_high, stack_high) + (
                dot(tile_high, stack_low) + dot(tile_low, stack_high)
            )


def forward(offs, pos, outer, inner, from_outer, from_inner, tiles):
    shape = jax.ShapeDtypeStruct(outer.shape, jnp.float32)
    rows, width = 2 * outer.shape[0], outer.shape[1]
    scratch = [VMEM((2 * rows, width), jnp.bfloat16)] * 2
    return call(
        forward_kernel, (shape, shape), (offs, pos, outer, inner, from_outer, from_inner, tiles),
        scratch, 6 * rows * BAND * TILE * width, 4 * (4 * rows * width), 2,
    )


def turn_kernel(parts, quarters, pos, *refs):
    *sources, high_out, low_out = refs
    turned = jnp.concatenate([ref[...].T for ref in sources], 1)
    high, low = split(turned)
    width = high.shape[0] // (parts * quarters)
    for d in range(parts):
        for e in range(quarters):
            for p in range(parts):
                for q in range(quarters):
                    @pl.when(jnp.logical_and((pos[0] + d) % parts == p, (pos[1] + e) % quarters == q))
                    def _(d=d, e=e, p=p, q=q):
                        here = (d * quarters + e) * width
                        there = (p * quarters + q) * width
                        high_out[here : here + width, :] = high[there : there + width]
                        low_out[here : here + width, :] = low[there : there + width]


def turn(parts, pos, sources):
    rows, width = sum(x.shape[0] for x in sources), sources[0].shape[1]
    half = jax.ShapeDtypeStruct((width, rows), jnp.bfloat16)
    return call(
        functools.partial(turn_kernel, parts, ORDERS), (half, half), (pos, *sources), (),
        width * width, 8 * width * rows, 1,
    )


def product_kernel(parts, high, low, *refs):
    sources, outs = refs[:-parts], refs[-parts:]
    right_high, right_low = split(jnp.concatenate([ref[...] for ref in sources], 0))
    rows = high.shape[0] // parts
    for d, out in enumerate(outs):
        here = pl.ds(d * rows, rows)
        a = high[here, :]
        out[...] = dot(a, right_high) + (dot(a, right_low) + dot(low[here, :], right_high))


def product(turned, sources, parts):
    high, low = turned
    rows, width = high.shape[0], sources[0].shape[1]
    shapes = tuple(jax.ShapeDtypeStruct((rows // parts, width), jnp.float32) for _ in range(parts))
    return call(
        functools.partial(product_kernel, parts), shapes, (high, low, *sources), (),
        6 * rows * width * high.shape[1], 4 * 4 * rows * width,
    )


def pick_kernel(count, pos, *refs):
    sources, outs = refs[: -count], refs[-count:]
    for d, out in enumerate(outs):
        power = (pos[1] + d) % count + pos[2]
        for k, ref in enumerate(sources):
            @pl.when(power == k)
            def _(out=out, ref=ref):
                out[...] = ref[...]


def place_kernel(scale, pos, *refs):
    *parts, out = refs
    count = len(parts)
    rows = parts[0].shape[0]
    for d, ref in enumerate(parts):
        at = (pos[1] + count - d) % count
        out[pl.ds(pl.multiple_of(at * rows, rows), rows), :] = ref[...] * scale


def local(rows_all, cols_all, ctrl, obsv, tiles, offs):
    total = rows_all * cols_all
    parts, splits = rows_all // ORDERS, cols_all // ORDERS
    r, c = lax.axis_index("row"), lax.axis_index("col")
    big_row, part, big_col, piece = r // parts, r % parts, c // splits, c % splits
    pos = jnp.stack([part, big_row, big_col, piece, r % 2]).astype(jnp.int32)
    devices = [(i, j) for i in range(rows_all) for j in range(cols_all)]

    def flat(i, j):
        return i * cols_all + j

    def permute(x, pairs):
        return lax.ppermute(x, AXES, pairs)

    def peers(move):
        return [(flat(i, j), flat(*move(i, j))) for i, j in devices]

    def seat(s):
        lane, q = divmod(s, 2 * cols_all)
        j = q // 2 if lane % 2 == 0 else cols_all - 1 - q // 2
        return flat(2 * lane + q % 2, j)

    seats = [seat(s) for s in range(total)]
    relay = [(s, seats[s]) for s in range(total)]
    inside = [(seats[s], seats[s ^ 1]) for s in range(total)]
    across = [(seats[s], seats[s + 1]) for s in range(1, total - 1, 2)]
    across += [(b, a) for a, b in across]

    margin = HALO * TILE
    width = ctrl.shape[1]
    quarter = width // (parts * ORDERS)

    def halves(x):
        first = (c % 2) * margin
        return (
            lax.dynamic_slice_in_dim(x, first, margin, 0),
            lax.dynamic_slice_in_dim(x, margin - first, margin, 0),
        )

    own_ctrl = ctrl
    own_obsv = obsv
    offs = permute(offs, relay)
    outer, inner = (permute(x, relay) for x in halves(ctrl))
    tiles = permute(tiles, relay)
    ready, tiles, offs = lax.optimization_barrier((obsv, tiles, offs))
    far = tuple(permute(x, relay) for x in halves(ready))
    near_turned = turn(parts, pos, (own_obsv,))
    far_turned = turn(parts, pos, far)

    def over_parts(blocks):
        kept = blocks[0]
        for d in range(1, parts):
            kept = kept + permute(
                blocks[d], peers(lambda i, j: ((i // parts) * parts + (i + d) % parts, j))
            )
        if splits == 1:
            return kept
        wide = kept.shape[1] // splits
        cut = [
            lax.dynamic_slice_in_dim(kept, ((piece + d) % splits) * wide, wide, 1)
            for d in range(splits)
        ]
        kept = cut[0]
        for d in range(1, splits):
            kept = kept + permute(
                cut[d], peers(lambda i, j: (i, (j // splits) * splits + (j + d) % splits))
            )
        return kept

    def turned(i, e):
        return ((i // parts + e) % ORDERS) * parts + i % parts

    def over_rows(block):
        kept = block[:, :quarter]
        for e in range(1, ORDERS):
            sent = block[:, e * quarter : (e + 1) * quarter]
            kept = kept + permute(sent, peers(lambda i, j: (turned(i, e), j)))
        return kept

    def line(moves):
        return [
            (flat(i, a * splits + s), flat(i, b * splits + s))
            for a, b in moves for i in range(rows_all) for s in range(splits)
        ]

    def over_cols(own, powers):
        low_k, high_k = min(powers), max(powers)
        last = 2 * ORDERS - 2
        first = []
        if high_k >= 1:
            first.append((0, 1))
        if low_k < last:
            first.append((3, 2))
        second = []
        if high_k >= 2:
            second.append((1, 2))
        if low_k <= last - 2:
            second.append((2, 1))
        third = []
        if low_k <= ORDERS - 1:
            third.append((1, 0))
        if high_k >= ORDERS - 1:
            third.append((2, 3))
        both = own + permute(own, line(first))
        both = both + permute(both, line(second))
        ends = permute(both, line(third))
        if (3, 2) not in first:
            ends = ends + jnp.where(big_col == 3, own, 0.0)
        outer = jnp.logical_or(big_col == 0, big_col == 3)
        return jnp.where(outer, ends, both)

    def over_top(own):
        got = own
        for a in range(ORDERS - 1):
            got = got + permute(own, line([(a, ORDERS - 1)]))
        return got

    sums, rows_done, kept = {}, {}, {}

    def reduce_ready():
        for group in ROW_GROUPS:
            if all(k in sums for k in group) and group[0] not in rows_done:
                done = over_rows(jnp.stack([sums[k] for k in group]))
                for at, k in enumerate(group):
                    rows_done[k] = done[at : at + 1]
        for group in COL_GROUPS:
            if all(k in rows_done for k in group) and group[0] not in kept:
                own = jnp.concatenate([rows_done[k] for k in group], 0)
                done = over_top(own) if group == (2 * ORDERS - 2,) else over_cols(own, group)
                for at, k in enumerate(group):
                    kept[k] = done[at]

    sums[0] = over_parts(product(near_turned, (own_ctrl,), parts))
    reduce_ready()
    for k in range(1, 2 * ORDERS - 1):
        from_inner, from_outer = permute(inner, inside), permute(outer, across)
        outer, inner = forward(offs, pos, outer, inner, from_outer, from_inner, tiles)
        sums[k] = over_parts(product(far_turned, (outer, inner), parts))
        reduce_ready()

    shape = kept[0].shape
    block = jax.ShapeDtypeStruct(shape, jnp.float32)
    sent = call(
        functools.partial(pick_kernel, ORDERS), (block,) * ORDERS,
        (pos, *[kept[k] for k in range(2 * ORDERS - 1)]), (), shape[0] * shape[1], 44 * shape[0] * shape[1], 1,
    )
    got = [sent[0]] + [permute(sent[d], peers(lambda i, j: (turned(i, d), j))) for d in range(1, ORDERS)]
    out = jax.ShapeDtypeStruct((ORDERS * shape[0], shape[1]), jnp.float32)
    scale = 1.0 / math.sqrt(ctrl.shape[0] * total)
    return call(
        functools.partial(place_kernel, scale), out, (pos, *got), (),
        shape[0] * shape[1], 32 * shape[0] * shape[1], 1,
    )


def solution(mesh):
    return jax.shard_map(
        functools.partial(local, mesh.shape["row"], mesh.shape["col"]),
        mesh=mesh,
        in_specs=(P(AXES, None),) * 4,
        out_specs=P("row", "col"),
        check_vma=False,
    )
```

```python
import functools
import math

import jax
import jax.numpy as jnp
from jax import lax
from jax.experimental import pallas as pl
from jax.experimental.pallas import tpu as pltpu
from jax.sharding import PartitionSpec as P

TILE = 128
HALO = 2
BAND = 3
ORDERS = 4
AXES = ("row", "col")
VMEM = pltpu.VMEM
GRANT = 16 * 2**20
ROW_GROUPS = ((0,), (1, 2), (3, 4), (5,), (6,))
COL_GROUPS = ((0, 1, 2), (3, 4), (5,), (6,))


def call(kernel, outs, ins, scratch=(), flops=0, bytes_=0, scalars=0):
    specs = [pl.BlockSpec(memory_space=pltpu.SMEM)] * scalars
    specs += [pl.BlockSpec(memory_space=VMEM)] * (len(ins) - scalars)
    return pl.pallas_call(
        kernel,
        out_shape=outs,
        in_specs=specs,
        out_specs=jax.tree.map(lambda _: pl.BlockSpec(memory_space=VMEM), outs),
        scratch_shapes=list(scratch),
        cost_estimate=pl.CostEstimate(flops=flops, bytes_accessed=bytes_, transcendentals=0),
        compiler_params=pltpu.CompilerParams(vmem_limit_bytes=GRANT),
    )(*ins)


def split(value):
    high = value.astype(jnp.bfloat16)
    return high, (value - high.astype(jnp.float32)).astype(jnp.bfloat16)


def dot(a, b):
    return jnp.dot(a, b, preferred_element_type=jnp.float32)


def forward_kernel(offs, pos, outer, inner, from_outer, from_inner, tiles, outer_out, inner_out, high, low):
    margin = HALO * TILE
    odd = pos[4]
    placed = ((from_outer, 3 * odd), (outer, 1 + odd), (inner, 2 - odd), (from_inner, 3 - 3 * odd))
    for ref, place in placed:
        here = pl.ds(pl.multiple_of(place * margin, margin), margin)
        high[here, :], low[here, :] = split(ref[...])
    for out, base in ((outer_out, HALO * odd), (inner_out, HALO * (1 - odd))):
        for i in range(HALO):
            index = base + i
            starts = [
                pl.multiple_of((index + HALO + offs[index, b]) * TILE, TILE) for b in range(BAND)
            ]
            stack_high = jnp.concatenate([high[pl.ds(s, TILE), :] for s in starts], 0)
            stack_low = jnp.concatenate([low[pl.ds(s, TILE), :] for s in starts], 0)
            tile_high, tile_low = split(tiles[pl.ds(pl.multiple_of(index * TILE, TILE), TILE), :])
            out[i * TILE : (i + 1) * TILE, :] = dot(tile_high, stack_high) + (
                dot(tile_high, stack_low) + dot(tile_low, stack_high)
            )


def forward(offs, pos, outer, inner, from_outer, from_inner, tiles):
    shape = jax.ShapeDtypeStruct(outer.shape, jnp.float32)
    rows, width = 2 * outer.shape[0], outer.shape[1]
    scratch = [VMEM((2 * rows, width), jnp.bfloat16)] * 2
    return call(
        forward_kernel, (shape, shape), (offs, pos, outer, inner, from_outer, from_inner, tiles),
        scratch, 6 * rows * BAND * TILE * width, 4 * (4 * rows * width), 2,
    )


def turn_kernel(parts, quarters, pos, *refs):
    *sources, high_out, low_out = refs
    turned = jnp.concatenate([ref[...].T for ref in sources], 1)
    high, low = split(turned)
    width = high.shape[0] // (parts * quarters)
    for d in range(parts):
        for e in range(quarters):
            for p in range(parts):
                for q in range(quarters):
                    @pl.when(jnp.logical_and((pos[0] + d) % parts == p, (pos[1] + e) % quarters == q))
                    def _(d=d, e=e, p=p, q=q):
                        here = (d * quarters + e) * width
                        there = (p * quarters + q) * width
                        high_out[here : here + width, :] = high[there : there + width]
                        low_out[here : here + width, :] = low[there : there + width]


def turn(parts, pos, sources):
    rows, width = sum(x.shape[0] for x in sources), sources[0].shape[1]
    half = jax.ShapeDtypeStruct((width, rows), jnp.bfloat16)
    return call(
        functools.partial(turn_kernel, parts, ORDERS), (half, half), (pos, *sources), (),
        width * width, 8 * width * rows, 1,
    )


def product_kernel(parts, high, low, *refs):
    sources, outs = refs[:-parts], refs[-parts:]
    right_high, right_low = split(jnp.concatenate([ref[...] for ref in sources], 0))
    rows = high.shape[0] // parts
    for d, out in enumerate(outs):
        here = pl.ds(d * rows, rows)
        a = high[here, :]
        out[...] = dot(a, right_high) + (dot(a, right_low) + dot(low[here, :], right_high))


def product(turned, sources, parts):
    high, low = turned
    rows, width = high.shape[0], sources[0].shape[1]
    shapes = tuple(jax.ShapeDtypeStruct((rows // parts, width), jnp.float32) for _ in range(parts))
    return call(
        functools.partial(product_kernel, parts), shapes, (high, low, *sources), (),
        6 * rows * width * high.shape[1], 4 * 4 * rows * width,
    )


def pick_kernel(count, pos, *refs):
    sources, outs = refs[: -count], refs[-count:]
    for d, out in enumerate(outs):
        power = (pos[1] + d) % count + pos[2]
        for k, ref in enumerate(sources):
            @pl.when(power == k)
            def _(out=out, ref=ref):
                out[...] = ref[...]


def place_kernel(scale, pos, *refs):
    *parts, out = refs
    count = len(parts)
    rows = parts[0].shape[0]
    for d, ref in enumerate(parts):
        at = (pos[1] + count - d) % count
        out[pl.ds(pl.multiple_of(at * rows, rows), rows), :] = ref[...] * scale


def local(rows_all, cols_all, ctrl, obsv, tiles, offs):
    total = rows_all * cols_all
    parts, splits = rows_all // ORDERS, cols_all // ORDERS
    r, c = lax.axis_index("row"), lax.axis_index("col")
    big_row, part, big_col, piece = r // parts, r % parts, c // splits, c % splits
    pos = jnp.stack([part, big_row, big_col, piece, r % 2]).astype(jnp.int32)
    devices = [(i, j) for i in range(rows_all) for j in range(cols_all)]

    def flat(i, j):
        return i * cols_all + j

    def permute(x, pairs):
        return lax.ppermute(x, AXES, pairs)

    def peers(move):
        return [(flat(i, j), flat(*move(i, j))) for i, j in devices]

    def seat(s):
        lane, q = divmod(s, 2 * cols_all)
        j = q // 2 if lane % 2 == 0 else cols_all - 1 - q // 2
        return flat(2 * lane + q % 2, j)

    seats = [seat(s) for s in range(total)]
    relay = [(s, seats[s]) for s in range(total)]
    inside = [(seats[s], seats[s ^ 1]) for s in range(total)]
    across = [(seats[s], seats[s + 1]) for s in range(1, total - 1, 2)]
    across += [(b, a) for a, b in across]

    margin = HALO * TILE
    width = ctrl.shape[1]
    quarter = width // (parts * ORDERS)

    def halves(x):
        first = (c % 2) * margin
        return (
            lax.dynamic_slice_in_dim(x, first, margin, 0),
            lax.dynamic_slice_in_dim(x, margin - first, margin, 0),
        )

    first, second = halves(ctrl)
    far_first, far_second = halves(obsv)
    moved_offs = permute(offs, relay)
    outer = permute(first, relay)
    inner = permute(second, relay)
    moved_tiles = permute(tiles, relay)
    far = (permute(far_first, relay), permute(far_second, relay))
    near_turned = turn(parts, pos, (obsv,))
    far_turned = turn(parts, pos, far)

    def over_parts(blocks):
        kept = blocks[0]
        for d in range(1, parts):
            move = peers(lambda i, j: ((i // parts) * parts + (i + d) % parts, j))
            kept = kept + permute(blocks[d], move)
        if splits == 1:
            return kept
        wide = kept.shape[1] // splits
        cut = [
            lax.dynamic_slice_in_dim(kept, ((piece + d) % splits) * wide, wide, 1)
            for d in range(splits)
        ]
        kept = cut[0]
        for d in range(1, splits):
            move = peers(lambda i, j: (i, (j // splits) * splits + (j + d) % splits))
            kept = kept + permute(cut[d], move)
        return kept

    def turned(i, e):
        return ((i // parts + e) % ORDERS) * parts + i % parts

    def over_rows(block):
        kept = block[:, :quarter]
        for e in range(1, ORDERS):
            sent = block[:, e * quarter : (e + 1) * quarter]
            kept = kept + permute(sent, peers(lambda i, j: (turned(i, e), j)))
        return kept

    def line(moves):
        return [
            (flat(i, a * splits + s), flat(i, b * splits + s))
            for a, b in moves for i in range(rows_all) for s in range(splits)
        ]

    def over_cols(own, powers):
        low_k, high_k = min(powers), max(powers)
        last = 2 * ORDERS - 2
        first = []
        if high_k >= 1:
            first.append((0, 1))
        if low_k < last:
            first.append((3, 2))
        second = []
        if high_k >= 2:
            second.append((1, 2))
        if low_k <= last - 2:
            second.append((2, 1))
        third = []
        if low_k <= ORDERS - 1:
            third.append((1, 0))
        if high_k >= ORDERS - 1:
            third.append((2, 3))
        both = own + permute(own, line(first))
        both = both + permute(both, line(second))
        ends = permute(both, line(third))
        if (3, 2) not in first:
            ends = ends + jnp.where(big_col == 3, own, 0.0)
        outer = jnp.logical_or(big_col == 0, big_col == 3)
        return jnp.where(outer, ends, both)

    def over_top(own):
        got = own
        for a in range(ORDERS - 1):
            got = got + permute(own, line([(a, ORDERS - 1)]))
        return got

    sums, rows_done, kept = {}, {}, {}

    def reduce_ready():
        for group in ROW_GROUPS:
            if all(k in sums for k in group) and group[0] not in rows_done:
                done = over_rows(jnp.stack([sums[k] for k in group]))
                for at, k in enumerate(group):
                    rows_done[k] = done[at : at + 1]
        for group in COL_GROUPS:
            if all(k in rows_done for k in group) and group[0] not in kept:
                own = jnp.concatenate([rows_done[k] for k in group], 0)
                done = over_top(own) if group == (2 * ORDERS - 2,) else over_cols(own, group)
                for at, k in enumerate(group):
                    kept[k] = done[at]

    sums[0] = over_parts(product(near_turned, (ctrl,), parts))
    reduce_ready()
    for k in range(1, 2 * ORDERS - 1):
        from_inner = permute(inner, inside)
        from_outer = permute(outer, across)
        outer, inner = forward(moved_offs, pos, outer, inner, from_outer, from_inner, moved_tiles)
        sums[k] = over_parts(product(far_turned, (outer, inner), parts))
        reduce_ready()

    shape = kept[0].shape
    block = jax.ShapeDtypeStruct(shape, jnp.float32)
    sent = call(
        functools.partial(pick_kernel, ORDERS), (block,) * ORDERS,
        (pos, *[kept[k] for k in range(2 * ORDERS - 1)]), (), shape[0] * shape[1], 44 * shape[0] * shape[1], 1,
    )
    got = [sent[0]] + [permute(sent[d], peers(lambda i, j: (turned(i, d), j))) for d in range(1, ORDERS)]
    out = jax.ShapeDtypeStruct((ORDERS * shape[0], shape[1]), jnp.float32)
    scale = 1.0 / math.sqrt(ctrl.shape[0] * total)
    return call(
        functools.partial(place_kernel, scale), out, (pos, *got), (),
        shape[0] * shape[1], 32 * shape[0] * shape[1], 1,
    )


def solution(mesh):
    rows_all, cols_all = mesh.shape["row"], mesh.shape["col"]

    def body(*args):
        return local(rows_all, cols_all, *args)

    return jax.shard_map(
        body,
        mesh=mesh,
        in_specs=(P(AXES, None),) * 4,
        out_specs=P("row", "col"),
        check_vma=False,
    )
```

```python
import functools
import math

import jax
import jax.numpy as jnp
from jax import lax
from jax.experimental import pallas as pl
from jax.experimental.pallas import tpu as pltpu
from jax.sharding import PartitionSpec as P

TILE = 128
HALO = 2
BAND = 3
ORDERS = 4
AXES = ("row", "col")
VMEM = pltpu.VMEM
GRANT = 16 * 2**20
ROW_GROUPS = ((0,), (1, 2), (3, 4), (5,), (6,))
COL_GROUPS = ((0, 1, 2), (3, 4), (5,), (6,))


def call(kernel, outs, ins, scratch=(), flops=0, bytes_=0, scalars=0):
    specs = [pl.BlockSpec(memory_space=pltpu.SMEM)] * scalars
    specs += [pl.BlockSpec(memory_space=VMEM)] * (len(ins) - scalars)
    return pl.pallas_call(
        kernel,
        out_shape=outs,
        in_specs=specs,
        out_specs=jax.tree.map(lambda _: pl.BlockSpec(memory_space=VMEM), outs),
        scratch_shapes=list(scratch),
        cost_estimate=pl.CostEstimate(flops=flops, bytes_accessed=bytes_, transcendentals=0),
        compiler_params=pltpu.CompilerParams(vmem_limit_bytes=GRANT),
    )(*ins)


def split(value):
    high = value.astype(jnp.bfloat16)
    return high, (value - high.astype(jnp.float32)).astype(jnp.bfloat16)


def dot(a, b):
    return jnp.dot(a, b, preferred_element_type=jnp.float32)


def forward_kernel(offs, pos, outer, inner, from_outer, from_inner, tiles, outer_out, inner_out, high, low):
    margin = HALO * TILE
    odd = pos[4]
    placed = ((from_outer, 3 * odd), (outer, 1 + odd), (inner, 2 - odd), (from_inner, 3 - 3 * odd))
    for ref, place in placed:
        here = pl.ds(pl.multiple_of(place * margin, margin), margin)
        high[here, :], low[here, :] = split(ref[...])
    for out, base in ((outer_out, HALO * odd), (inner_out, HALO * (1 - odd))):
        for i in range(HALO):
            index = base + i
            starts = [
                pl.multiple_of((index + HALO + offs[index, b]) * TILE, TILE) for b in range(BAND)
            ]
            stack_high = jnp.concatenate([high[pl.ds(s, TILE), :] for s in starts], 0)
            stack_low = jnp.concatenate([low[pl.ds(s, TILE), :] for s in starts], 0)
            tile_high, tile_low = split(tiles[pl.ds(pl.multiple_of(index * TILE, TILE), TILE), :])
            out[i * TILE : (i + 1) * TILE, :] = dot(tile_high, stack_high) + (
                dot(tile_high, stack_low) + dot(tile_low, stack_high)
            )


def forward(offs, pos, outer, inner, from_outer, from_inner, tiles):
    shape = jax.ShapeDtypeStruct(outer.shape, jnp.float32)
    rows, width = 2 * outer.shape[0], outer.shape[1]
    scratch = [VMEM((2 * rows, width), jnp.bfloat16)] * 2
    return call(
        forward_kernel, (shape, shape), (offs, pos, outer, inner, from_outer, from_inner, tiles),
        scratch, 6 * rows * BAND * TILE * width, 4 * (4 * rows * width), 2,
    )


def turn_kernel(parts, quarters, pos, *refs):
    *sources, high_out, low_out = refs
    turned = jnp.concatenate([ref[...].T for ref in sources], 1)
    high, low = split(turned)
    width = high.shape[0] // (parts * quarters)
    for d in range(parts):
        for e in range(quarters):
            for p in range(parts):
                for q in range(quarters):
                    @pl.when(jnp.logical_and((pos[0] + d) % parts == p, (pos[1] + e) % quarters == q))
                    def _(d=d, e=e, p=p, q=q):
                        here = (d * quarters + e) * width
                        there = (p * quarters + q) * width
                        high_out[here : here + width, :] = high[there : there + width]
                        low_out[here : here + width, :] = low[there : there + width]


def turn(parts, pos, sources):
    rows, width = sum(x.shape[0] for x in sources), sources[0].shape[1]
    half = jax.ShapeDtypeStruct((width, rows), jnp.bfloat16)
    return call(
        functools.partial(turn_kernel, parts, ORDERS), (half, half), (pos, *sources), (),
        width * width, 8 * width * rows, 1,
    )


def product_kernel(parts, high, low, *refs):
    sources, outs = refs[:-parts], refs[-parts:]
    right_high, right_low = split(jnp.concatenate([ref[...] for ref in sources], 0))
    rows = high.shape[0] // parts
    for d, out in enumerate(outs):
        here = pl.ds(d * rows, rows)
        a = high[here, :]
        out[...] = dot(a, right_high) + (dot(a, right_low) + dot(low[here, :], right_high))


def product(turned, sources, parts):
    high, low = turned
    rows, width = high.shape[0], sources[0].shape[1]
    shapes = tuple(jax.ShapeDtypeStruct((rows // parts, width), jnp.float32) for _ in range(parts))
    return call(
        functools.partial(product_kernel, parts), shapes, (high, low, *sources), (),
        6 * rows * width * high.shape[1], 4 * 4 * rows * width,
    )


def pick_kernel(count, pos, *refs):
    sources, outs = refs[: -count], refs[-count:]
    for d, out in enumerate(outs):
        power = (pos[1] + d) % count + pos[2]
        for k, ref in enumerate(sources):
            @pl.when(power == k)
            def _(out=out, ref=ref):
                out[...] = ref[...]


def place_kernel(scale, pos, *refs):
    *parts, out = refs
    count = len(parts)
    rows = parts[0].shape[0]
    for d, ref in enumerate(parts):
        at = (pos[1] + count - d) % count
        out[pl.ds(pl.multiple_of(at * rows, rows), rows), :] = ref[...] * scale


def local(rows_all, cols_all, ctrl, obsv, tiles, offs):
    total = rows_all * cols_all
    parts, splits = rows_all // ORDERS, cols_all // ORDERS
    r, c = lax.axis_index("row"), lax.axis_index("col")
    big_row, part, big_col, piece = r // parts, r % parts, c // splits, c % splits
    pos = jnp.stack([part, big_row, big_col, piece, r % 2]).astype(jnp.int32)
    devices = [(i, j) for i in range(rows_all) for j in range(cols_all)]

    def flat(i, j):
        return i * cols_all + j

    def permute(x, pairs):
        return lax.ppermute(x, AXES, pairs)

    def peers(move):
        return [(flat(i, j), flat(*move(i, j))) for i, j in devices]

    def seat(s):
        lane, q = divmod(s, 2 * cols_all)
        j = q // 2 if lane % 2 == 0 else cols_all - 1 - q // 2
        return flat(2 * lane + q % 2, j)

    seats = [seat(s) for s in range(total)]
    relay = [(s, seats[s]) for s in range(total)]
    inside = [(seats[s], seats[s ^ 1]) for s in range(total)]
    across = [(seats[s], seats[s + 1]) for s in range(1, total - 1, 2)]
    across += [(b, a) for a, b in across]

    margin = HALO * TILE
    width = ctrl.shape[1]
    quarter = width // (parts * ORDERS)

    def halves(x, odd):
        first = odd * margin
        return (
            lax.dynamic_slice_in_dim(x, first, margin, 0),
            lax.dynamic_slice_in_dim(x, margin - first, margin, 0),
        )

    moved_ctrl = permute(ctrl, relay)
    moved_offs = permute(offs, relay)
    moved_tiles = permute(tiles, relay)
    far_halves = halves(obsv, c % 2)
    far = tuple(permute(x, relay) for x in far_halves)
    outer, inner = halves(moved_ctrl, r % 2)
    near_turned = turn(parts, pos, (obsv,))
    far_turned = turn(parts, pos, far)

    def over_parts(blocks):
        kept = blocks[0]
        for d in range(1, parts):
            move = peers(lambda i, j: ((i // parts) * parts + (i + d) % parts, j))
            kept = kept + permute(blocks[d], move)
        if splits == 1:
            return kept
        wide = kept.shape[1] // splits
        cut = [
            lax.dynamic_slice_in_dim(kept, ((piece + d) % splits) * wide, wide, 1)
            for d in range(splits)
        ]
        kept = cut[0]
        for d in range(1, splits):
            move = peers(lambda i, j: (i, (j // splits) * splits + (j + d) % splits))
            kept = kept + permute(cut[d], move)
        return kept

    def turned(i, e):
        return ((i // parts + e) % ORDERS) * parts + i % parts

    def over_rows(block):
        kept = block[:, :quarter]
        for e in range(1, ORDERS):
            sent = block[:, e * quarter : (e + 1) * quarter]
            kept = kept + permute(sent, peers(lambda i, j: (turned(i, e), j)))
        return kept

    def line(moves):
        return [
            (flat(i, a * splits + s), flat(i, b * splits + s))
            for a, b in moves for i in range(rows_all) for s in range(splits)
        ]

    def over_cols(own, powers):
        low_k, high_k = min(powers), max(powers)
        last = 2 * ORDERS - 2
        first = []
        if high_k >= 1:
            first.append((0, 1))
        if low_k < last:
            first.append((3, 2))
        second = []
        if high_k >= 2:
            second.append((1, 2))
        if low_k <= last - 2:
            second.append((2, 1))
        third = []
        if low_k <= ORDERS - 1:
            third.append((1, 0))
        if high_k >= ORDERS - 1:
            third.append((2, 3))
        both = own + permute(own, line(first))
        both = both + permute(both, line(second))
        ends = permute(both, line(third))
        if (3, 2) not in first:
            ends = ends + jnp.where(big_col == 3, own, 0.0)
        outer = jnp.logical_or(big_col == 0, big_col == 3)
        return jnp.where(outer, ends, both)

    def over_top(own):
        got = own
        for a in range(ORDERS - 1):
            got = got + permute(own, line([(a, ORDERS - 1)]))
        return got

    sums, rows_done, kept = {}, {}, {}

    def reduce_ready():
        for group in ROW_GROUPS:
            if all(k in sums for k in group) and group[0] not in rows_done:
                done = over_rows(jnp.stack([sums[k] for k in group]))
                for at, k in enumerate(group):
                    rows_done[k] = done[at : at + 1]
        for group in COL_GROUPS:
            if all(k in rows_done for k in group) and group[0] not in kept:
                own = jnp.concatenate([rows_done[k] for k in group], 0)
                done = over_top(own) if group == (2 * ORDERS - 2,) else over_cols(own, group)
                for at, k in enumerate(group):
                    kept[k] = done[at]

    sums[0] = over_parts(product(near_turned, (ctrl,), parts))
    reduce_ready()
    for k in range(1, 2 * ORDERS - 1):
        from_inner = permute(inner, inside)
        from_outer = permute(outer, across)
        outer, inner = forward(moved_offs, pos, outer, inner, from_outer, from_inner, moved_tiles)
        sums[k] = over_parts(product(far_turned, (outer, inner), parts))
        reduce_ready()

    shape = kept[0].shape
    block = jax.ShapeDtypeStruct(shape, jnp.float32)
    sent = call(
        functools.partial(pick_kernel, ORDERS), (block,) * ORDERS,
        (pos, *[kept[k] for k in range(2 * ORDERS - 1)]), (), shape[0] * shape[1], 44 * shape[0] * shape[1], 1,
    )
    got = [sent[0]] + [permute(sent[d], peers(lambda i, j: (turned(i, d), j))) for d in range(1, ORDERS)]
    out = jax.ShapeDtypeStruct((ORDERS * shape[0], shape[1]), jnp.float32)
    scale = 1.0 / math.sqrt(ctrl.shape[0] * total)
    return call(
        functools.partial(place_kernel, scale), out, (pos, *got), (),
        shape[0] * shape[1], 32 * shape[0] * shape[1], 1,
    )


def solution(mesh):
    rows_all, cols_all = mesh.shape["row"], mesh.shape["col"]

    def body(*args):
        return local(rows_all, cols_all, *args)

    return jax.shard_map(
        body,
        mesh=mesh,
        in_specs=(P(AXES, None),) * 4,
        out_specs=P("row", "col"),
        check_vma=False,
    )
```
